32 devices in a mesh: px: 4 (over x, core), py: 8 (over z, y).
Axes of the slice: x: 2, y: 2, z: 4, core: 2. Of those that a mesh axis runs over, the one named last changes fastest.
Arguments:
- metric: bfloat16 [3, 160, 24, 1024], P(None, 'px', None, 'py'), may hold values from 0.25 to 24
- helmholtz: bfloat16 [160, 24, 1024], P('px', None, 'py'), may hold values from 1 to 30
- forcing: bfloat16 [160, 24, 1024], P('px', None, 'py'), may hold values from -6 to 6
- orientation: int32 [160, 1024], P('px', 'py'), may hold values 0 or 1
- start_x: float32 [160, 24, 1024], P('px', None, 'py'), may hold values from -6 to 6
- start_y: float32 [160, 24, 1024], P('px', None, 'py'), may hold values from -6 to 6
- start_z: float32 [160, 25, 1024], P('px', None, 'py'), may hold values from -6 to 6
Outputs:
- trace_x: float32 [160, 24, 1024], P('px', None, 'py')
- trace_y: float32 [160, 24, 1024], P('px', None, 'py')
- trace_z: float32 [160, 25, 1024], P('px', None, 'py')
- pressure: float32 [160, 24, 1024], P('px', None, 'py')
The draws below stay inside these ranges and needn't reach their ends.
All inputs are finite; a program needn't handle non-finite values. No bound on the sum of `orientation` on one device may be relied on, other than what follows from the above.
Results may differ from the reference program's by a relative error of at most 0.0003.
Values sent between devices are 32-bit elements; how exact they have to be, the bound alone decides.
A program may use at most 64 MiB of HBM per device.

```python
import math
import jax
import jax.numpy as jnp

L = 24
ITERS = 2
NX = 160
NY = 1024


def draw_metric(key, part):
    uniform_base = jax.random.uniform(key, (3, NX, L, NY), jnp.float32)
    across = (jnp.arange(NX, dtype=jnp.float32) / NX)[None, :, None, None]
    sideways = (jnp.arange(NY, dtype=jnp.float32) / NY)[None, None, None, :]
    tilt_factor = 3.0 ** across * 1.5 ** sideways
    spread = 0.5 * 8.0 ** uniform_base
    return (spread * tilt_factor).astype(jnp.bfloat16)


def set_ends(drawn, key, smallest, largest):
    extent = drawn.shape
    place = [jax.random.randint(jax.random.fold_in(key, axis), (), 0, extent[axis]) for axis in range(len(extent))]
    drawn = drawn.at[tuple(place)].set(smallest)
    longest = extent.index(max(extent))
    place[longest] = (place[longest] + 1) % extent[longest]
    return drawn.at[tuple(place)].set(largest)


def shard_levels(rng, extent, cuts, low, high):
    gain, own = 1.0, jax.random.fold_in(rng, 6)
    for dim, blocks in cuts:
        heights = jnp.exp(jax.random.uniform(jax.random.fold_in(own, dim), (blocks,), jnp.float32, low / len(cuts), high / len(cuts)))
        gain = gain * jnp.repeat(heights, extent[dim] // blocks).reshape([-1 if axis == dim else 1 for axis in range(len(extent))])
    return gain


def normal_values(key, shape, scale, most, shards=(), held_as=jnp.bfloat16):
    gain = shard_levels(key, shape, shards, -0.22, 0.18) if shards else 1.0
    array = jax.random.normal(key, shape, jnp.float32) * scale * gain
    return jnp.minimum(jnp.maximum(array, -most), most).astype(held_as)


def setup_inputs(seed: int = 0) -> dict:
    keys = jax.random.split(jax.random.key(seed), 8)
    return {
        "metric": draw_metric(jax.random.fold_in(keys[7], 71), 0),
        "helmholtz": jnp.clip(jnp.exp(math.log(30.0) - 3.4011974 * jax.random.uniform(keys[1], (NX, L, NY), jnp.float32) ** shard_levels(keys[1], (NX, L, NY), ((0, 4), (2, 8)), -0.2, 0.2)), 1.0, 30.0).astype(jnp.bfloat16),
        "forcing": normal_values(keys[2], (NX, L, NY), 1.0, 6.0, ((0, 4), (2, 8))),
        "orientation": set_ends((jax.random.randint(keys[3], (NX, NY), 0, 2) < 1).astype(jnp.int32), jax.random.fold_in(keys[3], 1), 0, 1),
        "start_x": normal_values(keys[4], (NX, L, NY), 1.0, 6.0, ((0, 4), (2, 8)), jnp.float32),
        "start_y": normal_values(keys[5], (NX, L, NY), 1.0, 6.0, ((0, 4), (2, 8)), jnp.float32),
        "start_z": normal_values(keys[6], (NX, L + 1, NY), 1.0, 6.0, ((0, 4), (2, 8)), jnp.float32),
    }


def coefficients(metric, helmholtz, orientation):
    metric_x = metric[0].astype(jnp.float32)
    metric_y = metric[1].astype(jnp.float32)
    metric_z = metric[2].astype(jnp.float32)
    turned = (orientation == 1)[:, None, :]
    inverse_x = 1.0 / jnp.where(turned, metric_y, metric_x)
    inverse_y = 1.0 / jnp.where(turned, metric_x, metric_y)
    inverse_z = 1.0 / metric_z
    denominator = helmholtz.astype(jnp.float32) + 2.0 * (3.0 * inverse_x + 3.0 * inverse_y + 3.0 * inverse_z)
    return (inverse_x, inverse_y, inverse_z, denominator)


def element(trace_west, trace_east, trace_south, trace_north, trace_bottom, trace_top, coeffs, source):
    inverse_x, inverse_y, inverse_z, denominator = coeffs
    weight_x = 3.0 * inverse_x
    weight_y = 3.0 * inverse_y
    weight_z = 3.0 * inverse_z
    gathered = weight_x * (trace_west + trace_east) + weight_y * (trace_south + trace_north) + weight_z * (trace_bottom + trace_top)
    pressure = (source + gathered) / denominator
    flux_west = inverse_x * (2.0 * trace_west + trace_east) - weight_x * pressure
    flux_east = inverse_x * (trace_west + 2.0 * trace_east) - weight_x * pressure
    flux_south = inverse_y * (2.0 * trace_south + trace_north) - weight_y * pressure
    flux_north = inverse_y * (trace_south + 2.0 * trace_north) - weight_y * pressure
    flux_bottom = inverse_z * (2.0 * trace_bottom + trace_top) - weight_z * pressure
    flux_top = inverse_z * (trace_bottom + 2.0 * trace_top) - weight_z * pressure
    return (flux_west, flux_east, flux_south, flux_north, flux_bottom, flux_top, pressure)


def stack_vertical(flux_bottom, flux_top):
    zero_layer = jnp.zeros_like(flux_bottom[:, :1])
    return jnp.concatenate([flux_bottom, zero_layer], 1) + jnp.concatenate([zero_layer, flux_top], 1)


def assemble(fields, coeffs, source):
    field_x, field_y, field_z = fields
    east_side = jnp.roll(field_x, -1, 0)
    north_side = jnp.roll(field_y, -1, 2)
    fluxes = element(field_x, east_side, field_y, north_side, field_z[:, :-1], field_z[:, 1:], coeffs, source)
    sum_x = fluxes[0] + jnp.roll(fluxes[1], 1, 0)
    sum_y = fluxes[2] + jnp.roll(fluxes[3], 1, 2)
    sum_z = stack_vertical(fluxes[4], fluxes[5])
    return (sum_x, sum_y, sum_z), fluxes[6]


def inner(first_vec, second_vec):
    return jnp.sum(first_vec[0] * second_vec[0]) + jnp.sum(first_vec[1] * second_vec[1]) + jnp.sum(first_vec[2] * second_vec[2])


def combine(first_vec, scale, second_vec):
    return tuple(member + scale * other for member, other in zip(first_vec, second_vec))


def reference(metric, helmholtz, forcing, orientation, start_x, start_y, start_z):
    coeffs = coefficients(metric, helmholtz, orientation)
    source = forcing.astype(jnp.float32)
    traces = (start_x, start_y, start_z)
    sums, unused = assemble(traces, coeffs, source)
    residual = tuple(-member for member in sums)
    direction = residual
    norm_now = inner(residual, residual)
    for iteration in range(ITERS):
        applied, unused = assemble(direction, coeffs, 0.0)
        step_size = norm_now / inner(direction, applied)
        traces = combine(traces, step_size, direction)
        residual = combine(residual, -step_size, applied)
        if iteration + 1 < ITERS:
            norm_next = inner(residual, residual)
            direction = combine(residual, norm_next / norm_now, direction)
            norm_now = norm_next
    unused, pressure = assemble(traces, coeffs, source)
    return (traces[0], traces[1], traces[2], pressure)
```

```python
import functools

import jax
import jax.numpy as jnp
from jax import lax
from jax.experimental import pallas as pl
from jax.experimental.pallas import tpu as pltpu
from jax.sharding import PartitionSpec as P

MESH = pl.DeviceIdType.MESH
F32 = jnp.float32


def fold(x):
    total = x[0:8]
    for row in range(8, x.shape[0], 8):
        total = total + x[row : row + 8]
    return total


def kernel(
    npx, npy,
    met_h, hel_h, src_h, ori_h, sx_h, sy_h, sz_h,
    ox, oy, oz, op,
    met, hel, src, ori, xs, ys, zs,
    ix, iy, iz, di, p0, p1, p2, rx, ry, rz, vx, vy, vz,
    strip, nsend1, esend1, nsend2, esend2,
    hy, cx, cy, nrecv1, erecv1, nrecv2, erecv2,
    mom, slots1, slots2,
    in_sem, send_sem, recv_sem,
):
    nx, levels, ny = hel.shape
    unroll = next(u for u in (8, 5, 4, 2, 1) if nx % u == 0)
    px, py = lax.axis_index("px"), lax.axis_index("py")

    def device(dx, dy):
        return (lax.rem(px + dx + npx, npx), lax.rem(py + dy + npy, npy))

    loads = []
    for n, (a, b) in enumerate(
        (
            (sx_h, xs.at[pl.ds(0, nx)]), (sy_h, ys), (met_h, met), (ori_h, ori),
            (hel_h, hel), (src_h, src), (sz_h, zs),
        )
    ):
        copy = pltpu.make_async_copy(a, b, in_sem.at[n])
        copy.start()
        loads.append(copy)

    offsets = {(1, 0), (-1, 0), (0, 1), (0, -1), (-1, 1), (1, -1)}
    offsets |= {(d, 0) for d in range(1, npx)} | {(0, d) for d in range(1, npy)}
    offsets = sorted({(a % npx, b % npy) for a, b in offsets} - {(0, 0)})
    barrier = pltpu.get_barrier_semaphore()
    for a, b in offsets:
        pl.semaphore_signal(barrier, inc=1, device_id=device(a, b), device_id_type=MESH)
    pl.semaphore_wait(barrier, len(offsets))

    count = [0]
    sent = []

    def send(source, target, dx, dy):
        n = count[0]
        count[0] += 1
        copy = pltpu.make_async_remote_copy(
            src_ref=source, dst_ref=target, send_sem=send_sem.at[n], recv_sem=recv_sem.at[n],
            device_id=device(dx, dy), device_id_type=MESH,
        )
        copy.start()
        sent.append(copy)
        return copy

    lane = lax.broadcasted_iota(jnp.int32, (levels, ny), 1)
    first, last = lane == 0, lane == ny - 1
    zero = jnp.zeros((levels, ny), F32)
    zero8 = jnp.zeros((8, ny), F32)

    def loop(body, carry):
        def block(b, carry):
            for u in range(unroll):
                carry = body(b * unroll + u, carry)
            return carry

        return lax.fori_loop(0, nx // unroll, block, carry)

    def pack_first(i, y, held):
        return jnp.where(lane == i, pltpu.roll(y, i, 1), held)

    def pack_last(i, y, held):
        return jnp.where(lane == i, pltpu.roll(y, i + 1, 1), held)

    def partial(i, xf, yf, zf, a, b, c, d, source):
        w = xf[i]
        e = jnp.where(i < nx - 1, xf[jnp.minimum(i + 1, nx - 1)], 0.0)
        s = yf[i]
        n = jnp.where(last, 0.0, pltpu.roll(s, ny - 1, 1))
        bottom, top = zf[i, pl.ds(0, levels), :], zf[i, pl.ds(1, levels), :]
        total = 3.0 * (a * (w + e) + b * (s + n) + c * (bottom + top))
        if source is not None:
            total = total + source
        return total * d

    def complete(phase, xf, yf, zf, pf, coming, nb, eb, nco, eco):
        for copy in coming:
            copy.wait_recv()
        end = nx - 1
        pf[end] = pf[end] + 3.0 * ix[end] * di[end] * xf[nx]
        mine = strip[phase]
        iyh, kh = nco[2], nco[3]
        north_p = nb[1] + kh * mine + jnp.where(
            lane == end, pltpu.roll(kh, ny - 1, 1) * pltpu.roll(cx[phase], nx, 1), 0.0
        )
        flux_strip = iyh * (2.0 * mine + nb[0] - 3.0 * north_p)
        e = xf[0]
        west_p = eb[1] + eco[3] * e + jnp.where(
            last, eco[4] * pltpu.roll(cy[phase], ny - nx, 1), 0.0
        )
        flux_west_halo = eco[2] * (2.0 * e + eb[0] - 3.0 * west_p)
        north_strip = hy[phase]

        def column(i, flux_east):
            w, e, s = xf[i], xf[i + 1], yf[i]
            bottom, top = zf[i, pl.ds(0, levels), :], zf[i, pl.ds(1, levels), :]
            a, b, c = ix[i], iy[i], iz[i]
            halo = pltpu.roll(north_strip, ny - 1 - i, 1)
            n = jnp.where(last, halo, pltpu.roll(s, ny - 1, 1))
            p = pf[i] + jnp.where(last, 3.0 * b * di[i] * halo, 0.0)
            pf[i] = p
            sumx, sumy, sumz = w + e - 3.0 * p, s + n - 3.0 * p, bottom + top - 3.0 * p
            fx = a * (w + sumx) + flux_east
            flux_east = a * (e + sumx)
            north = pltpu.roll(b * (n + sumy), 1, 1)
            fy = b * (s + sumy) + jnp.where(
                first, pltpu.roll(flux_strip, lax.rem(ny - i, ny), 1), north
            )
            fz = jnp.concatenate([c * (bottom + sumz), zero8], 0) + pltpu.roll(
                jnp.concatenate([c * (top + sumz), zero8], 0), 1, 0
            )
            return fx, fy, fz, flux_east

        return column, flux_west_halo

    loads[0].wait()
    coming = [send(xs.at[0], xs.at[nx], -1, 0), send(xs.at[0], cx.at[0], -1, 1)]
    for copy in loads[1:]:
        copy.wait()

    def body(i, held):
        h0, s1, q1, b1, k1 = held
        turned = ori[pl.ds(i, 1), :] == 1
        mx, my, mz = met[0, i].astype(F32), met[1, i].astype(F32), met[2, i].astype(F32)
        a = 1.0 / jnp.where(turned, my, mx)
        b = 1.0 / jnp.where(turned, mx, my)
        c = 1.0 / mz
        d = 1.0 / (hel[i].astype(F32) + 6.0 * (a + b + c))
        ix[i], iy[i], iz[i], di[i] = a, b, c, d
        p = partial(i, xs, ys, zs, a, b, c, d, src[i].astype(F32))
        p0[i] = p
        s = ys[i]
        return (
            pack_first(i, s, h0), pack_last(i, s, s1), pack_last(i, p, q1),
            pack_last(i, b, b1), pack_last(i, 3.0 * b * d, k1),
        )

    h0, s1, q1, b1, k1 = loop(body, (zero,) * 5)
    end = nx - 1
    kx_end = 3.0 * ix[end] * di[end]
    strip[0] = h0
    nsend1[0], nsend1[1], nsend1[2] = s1, q1, b1
    nsend1[3] = pack_last(nx, kx_end, k1)
    esend1[0], esend1[1], esend1[2] = xs[end], p0[end], ix[end]
    esend1[3], esend1[4] = kx_end, 3.0 * iy[end] * di[end]
    coming += [
        send(esend1, erecv1, 1, 0), send(nsend1, nrecv1, 0, 1),
        send(strip.at[0], hy.at[0], 0, -1), send(strip.at[0], cy.at[0], 1, -1),
    ]

    column, flux = complete(0, xs, ys, zs, p0, coming, nrecv1, erecv1, nrecv1, erecv1)

    def body(i, held):
        flux, h0, s1, m0 = held
        fx, fy, fz, flux = column(i, flux)
        fx, fy, fz = -fx, -fy, -fz
        rx[i], ry[i], rz[i] = fx, fy, fz
        m0 = m0 + fold(fx * fx + fy * fy) + fold(fz * fz)
        return flux, pack_first(i, fy, h0), pack_last(i, fy, s1), m0

    flux, h0, s1, m0 = loop(body, (flux, zero, zero, zero8))
    strip[1] = h0
    nsend2[0] = s1
    esend2[0] = rx[end]
    coming = [
        send(rx.at[0], rx.at[nx], -1, 0), send(rx.at[0], cx.at[1], -1, 1),
        send(strip.at[1], hy.at[1], 0, -1), send(strip.at[1], cy.at[1], 1, -1),
    ]

    def body(i, q1):
        p = partial(i, rx, ry, rz, ix[i], iy[i], iz[i], di[i], None)
        p1[i] = p
        return pack_last(i, p, q1)

    q1 = loop(body, zero)
    nsend2[1] = q1
    esend2[1] = p1[end]
    coming += [send(esend2, erecv2, 1, 0), send(nsend2, nrecv2, 0, 1)]
    column, flux = complete(1, rx, ry, rz, p1, coming, nrecv2, erecv2, nrecv1, erecv1)

    def body(i, held):
        flux, h0, m1, m2 = held
        fx, fy, fz, flux = column(i, flux)
        vx[i], vy[i], vz[i] = fx, fy, fz
        m1 = m1 + fold(fx * rx[i] + fy * ry[i]) + fold(fz * rz[i])
        m2 = m2 + fold(fx * fx + fy * fy) + fold(fz * fz)
        return flux, pack_first(i, fy, h0), m1, m2

    flux, h0, m1, m2 = loop(body, (flux, zero, zero8, zero8))
    strip[2] = h0
    coming = [send(vx.at[0], vx.at[nx], -1, 0), send(strip.at[2], hy.at[2], 0, -1)]
    for copy in coming:
        copy.wait_recv()

    north_strip = hy[2]

    def body(i, m3):
        w, e, s = vx[i], vx[i + 1], vy[i]
        bottom, top = vz[i, pl.ds(0, levels), :], vz[i, pl.ds(1, levels), :]
        a, b, c = ix[i], iy[i], iz[i]
        n = jnp.where(last, pltpu.roll(north_strip, ny - 1 - i, 1), pltpu.roll(s, ny - 1, 1))
        sumx, sumy, sumz = w + e, s + n, bottom + top
        total = 3.0 * (a * sumx + b * sumy + c * sumz)
        p = total * di[i]
        p2[i] = p
        energy = (
            a * (w * w + e * e + sumx * sumx)
            + b * (s * s + n * n + sumy * sumy)
            + c * (bottom * bottom + top * top + sumz * sumz)
            - p * total
        )
        return m3 + fold(energy)

    m3 = loop(body, zero8)

    row = lax.broadcasted_iota(jnp.int32, (8, ny), 0)
    mine = zero8
    for n, m in enumerate((m0, m1, m2, m3)):
        mine = jnp.where(row == n, jnp.sum(m, 0, keepdims=True), mine)
    mom[0] = mine
    coming = [send(mom.at[0], slots1.at[d], d, 0) for d in range(1, npx)]
    for d, copy in enumerate(coming):
        copy.wait_recv()
        mine = mine + slots1[d + 1]
    mom[1] = mine
    coming = [send(mom.at[1], slots2.at[d], 0, d) for d in range(1, npy)]
    for d, copy in enumerate(coming):
        copy.wait_recv()
        mine = mine + slots2[d + 1]
    mine = jnp.sum(mine, 1, keepdims=True)
    m0, m1, m2, m3 = mine[0:1], mine[1:2], mine[2:3], mine[3:4]
    a0 = m0 / m1
    new = a0 * a0 * m2 - m0
    grown = 1.0 + new / m0
    curve = a0 * (a0 * m3 - grown * m2)
    good = (new > 0.0) & (curve > 0.0)
    a1 = jnp.where(good, new / jnp.where(good, curve, 1.0), 0.0)
    c0 = a0 + a1 * grown
    c1 = -a0 * a1
    c0 = jnp.broadcast_to(c0, (1, ny))
    c1 = jnp.broadcast_to(c1, (1, ny))

    def body(i, carry):
        ox[i] = xs[i] + c0 * rx[i] + c1 * vx[i]
        oy[i] = ys[i] + c0 * ry[i] + c1 * vy[i]
        faces = pl.ds(0, levels + 1)
        oz[i] = zs[i] + c0 * rz[i, faces, :] + c1 * vz[i, faces, :]
        op[i] = p0[i] + c0 * p1[i] + c1 * p2[i]
        return carry

    loop(body, 0)
    for copy in sent:
        copy.wait_send()


def local(npx, npy, metric, helmholtz, forcing, orientation, start_x, start_y, start_z):
    nx, levels, ny = start_x.shape
    faces = levels + 8
    cells = pltpu.VMEM((nx, levels, ny), F32)
    padded = pltpu.VMEM((nx + 1, levels, ny), F32)
    vertical = pltpu.VMEM((nx, faces, ny), F32)

    def tiles(n):
        return pltpu.VMEM((n, levels, ny), F32)

    sends = 14 + (npx - 1) + (npy - 1)
    return pl.pallas_call(
        functools.partial(kernel, npx, npy),
        out_shape=[jax.ShapeDtypeStruct(a.shape, F32) for a in (start_x, start_y, start_z, start_x)],
        in_specs=[pl.BlockSpec(memory_space=pl.ANY)] * 7,
        out_specs=[pl.BlockSpec(memory_space=pltpu.VMEM)] * 4,
        scratch_shapes=[
            pltpu.VMEM(metric.shape, metric.dtype),
            pltpu.VMEM(helmholtz.shape, helmholtz.dtype),
            pltpu.VMEM(forcing.shape, forcing.dtype),
            pltpu.VMEM(orientation.shape, orientation.dtype),
            padded, cells, pltpu.VMEM(start_z.shape, F32),
            cells, cells, cells, cells, cells, cells, cells,
            padded, cells, vertical, padded, cells, vertical,
            tiles(3), tiles(4), tiles(5), tiles(2), tiles(2),
            tiles(3), tiles(2), tiles(2), tiles(4), tiles(5), tiles(2), tiles(2),
            pltpu.VMEM((2, 8, ny), F32),
            pltpu.VMEM((npx, 8, ny), F32),
            pltpu.VMEM((npy, 8, ny), F32),
            pltpu.SemaphoreType.DMA((7,)),
            pltpu.SemaphoreType.DMA((sends,)),
            pltpu.SemaphoreType.DMA((sends,)),
        ],
        compiler_params=pltpu.CompilerParams(
            collective_id=0, has_side_effects=True, vmem_limit_bytes=40 * 1024 * 1024
        ),
    )(metric, helmholtz, forcing, orientation, start_x, start_y, start_z)


def solution(mesh):
    return jax.shard_map(
        functools.partial(local, mesh.shape["px"], mesh.shape["py"]),
        mesh=mesh,
        in_specs=(
            P(None, "px", None, "py"),
            P("px", None, "py"),
            P("px", None, "py"),
            P("px", "py"),
            P("px", None, "py"),
            P("px", None, "py"),
            P("px", None, "py"),
        ),
        out_specs=(P("px", None, "py"),) * 4,
        check_vma=False,
    )
```

```python
import functools

import jax
import jax.numpy as jnp
from jax import lax
from jax.experimental import pallas as pl
from jax.experimental.pallas import tpu as pltpu
from jax.sharding import PartitionSpec as P

MESH = pl.DeviceIdType.MESH
F32 = jnp.float32
DIRECT = 64


def fold(x):
    total = x[0:8]
    for row in range(8, x.shape[0], 8):
        total = total + x[row : row + 8]
    return total


def kernel(
    npx, npy,
    met_h, hel_h, src_h, ori_h, sx_h, sy_h, sz_h,
    ox, oy, oz, op,
    met, hel, src, ori, xs, ys, zs,
    ix, iy, iz, di, p0, p1, p2, rx, ry, rz, vx, vy, vz,
    strip, nsend1, esend1, nsend2, esend2,
    hy, cx, cy, nrecv1, erecv1, nrecv2, erecv2,
    mom, slots1, slots2,
    in_sem, z_sem, out_sem, send_sem, recv_sem, all_sem,
):
    nx, levels, ny = hel.shape
    direct = npx * npy <= DIRECT
    unroll = next(u for u in (10, 8, 5, 4, 2, 1) if nx % u == 0)
    px, py = lax.axis_index("px"), lax.axis_index("py")

    def device(dx, dy):
        return (lax.rem(px + dx + npx, npx), lax.rem(py + dy + npy, npy))

    loads = []
    for n, (a, b) in enumerate(
        (
            (sx_h, xs.at[pl.ds(0, nx)]), (sy_h, ys), (met_h, met), (ori_h, ori),
            (hel_h, hel), (src_h, src),
        )
    ):
        copy = pltpu.make_async_copy(a, b, in_sem.at[n])
        copy.start()
        loads.append(copy)
    for level in range(levels + 1):
        copy = pltpu.make_async_copy(sz_h.at[level], zs.at[:, level, :], z_sem.at[level])
        copy.start()
        loads.append(copy)

    offsets = {(1, 0), (-1, 0), (0, 1), (0, -1), (-1, 1), (1, -1)}
    offsets |= {(d, 0) for d in range(1, npx)} | {(0, d) for d in range(1, npy)}
    if direct:
        offsets = {(a, b) for a in range(npx) for b in range(npy)}
    offsets = sorted({(a % npx, b % npy) for a, b in offsets} - {(0, 0)})
    barrier = pltpu.get_barrier_semaphore()
    for a, b in offsets:
        pl.semaphore_signal(barrier, inc=1, device_id=device(a, b), device_id_type=MESH)

    count = [0]
    sent = []

    def send(source, target, dx, dy):
        n = count[0]
        count[0] += 1
        copy = pltpu.make_async_remote_copy(
            src_ref=source, dst_ref=target, send_sem=send_sem.at[n], recv_sem=recv_sem.at[n],
            device_id=device(dx, dy), device_id_type=MESH,
        )
        copy.start()
        sent.append(copy)
        return copy

    lane = lax.broadcasted_iota(jnp.int32, (levels, ny), 1)
    first, last = lane == 0, lane == ny - 1
    zero = jnp.zeros((levels, ny), F32)
    zero8 = jnp.zeros((8, ny), F32)

    def loop(body, carry):
        def block(b, carry):
            for u in range(unroll):
                carry = body(b * unroll + u, carry)
            return carry

        return lax.fori_loop(0, nx // unroll, block, carry)

    def pack_first(i, y, held):
        return jnp.where(lane == i, pltpu.roll(y, i, 1), held)

    def pack_last(i, y, held):
        return jnp.where(lane == i, pltpu.roll(y, i + 1, 1), held)

    def partial(i, xf, yf, zf, a, b, c, d, source):
        w = xf[i]
        e = jnp.where(i < nx - 1, xf[jnp.minimum(i + 1, nx - 1)], 0.0)
        s = yf[i]
        n = jnp.where(last, 0.0, pltpu.roll(s, ny - 1, 1))
        bottom, top = zf[i, pl.ds(0, levels), :], zf[i, pl.ds(1, levels), :]
        total = 3.0 * (a * (w + e) + b * (s + n) + c * (bottom + top))
        if source is not None:
            total = total + source
        return total * d

    def complete(phase, xf, yf, zf, pf, coming, nb, eb, nco, eco):
        for copy in coming:
            copy.wait_recv()
        end = nx - 1
        pf[end] = pf[end] + 3.0 * ix[end] * di[end] * xf[nx]
        mine = strip[phase]
        iyh, kh = nco[2], nco[3]
        north_p = nb[1] + kh * mine + jnp.where(
            lane == end, pltpu.roll(kh, ny - 1, 1) * pltpu.roll(cx[phase], nx, 1), 0.0
        )
        flux_strip = iyh * (2.0 * mine + nb[0] - 3.0 * north_p)
        e = xf[0]
        west_p = eb[1] + eco[3] * e + jnp.where(
            last, eco[4] * pltpu.roll(cy[phase], ny - nx, 1), 0.0
        )
        flux_west_halo = eco[2] * (2.0 * e + eb[0] - 3.0 * west_p)
        north_strip = hy[phase]

        def column(i, flux_east):
            w, e, s = xf[i], xf[i + 1], yf[i]
            bottom, top = zf[i, pl.ds(0, levels), :], zf[i, pl.ds(1, levels), :]
            a, b, c = ix[i], iy[i], iz[i]
            halo = pltpu.roll(north_strip, ny - 1 - i, 1)
            n = jnp.where(last, halo, pltpu.roll(s, ny - 1, 1))
            p = pf[i] + jnp.where(last, 3.0 * b * di[i] * halo, 0.0)
            pf[i] = p
            sumx, sumy, sumz = w + e - 3.0 * p, s + n - 3.0 * p, bottom + top - 3.0 * p
            fx = a * (w + sumx) + flux_east
            flux_east = a * (e + sumx)
            north = pltpu.roll(b * (n + sumy), 1, 1)
            fy = b * (s + sumy) + jnp.where(
                first, pltpu.roll(flux_strip, lax.rem(ny - i, ny), 1), north
            )
            fz = jnp.concatenate([c * (bottom + sumz), zero8], 0) + pltpu.roll(
                jnp.concatenate([c * (top + sumz), zero8], 0), 1, 0
            )
            return fx, fy, fz, flux_east

        return column, flux_west_halo

    for copy in loads:
        copy.wait()

    def body(i, held):
        h0, s1, q1, b1, k1 = held
        turned = ori[pl.ds(i, 1), :] == 1
        mx, my, mz = met[0, i].astype(F32), met[1, i].astype(F32), met[2, i].astype(F32)
        a = 1.0 / jnp.where(turned, my, mx)
        b = 1.0 / jnp.where(turned, mx, my)
        c = 1.0 / mz
        d = 1.0 / (hel[i].astype(F32) + 6.0 * (a + b + c))
        ix[i], iy[i], iz[i], di[i] = a, b, c, d
        p = partial(i, xs, ys, zs, a, b, c, d, src[i].astype(F32))
        p0[i] = p
        s = ys[i]
        return (
            pack_first(i, s, h0), pack_last(i, s, s1), pack_last(i, p, q1),
            pack_last(i, b, b1), pack_last(i, 3.0 * b * d, k1),
        )

    h0, s1, q1, b1, k1 = loop(body, (zero,) * 5)
    end = nx - 1
    kx_end = 3.0 * ix[end] * di[end]
    strip[0] = h0
    nsend1[0], nsend1[1], nsend1[2] = s1, q1, b1
    nsend1[3] = pack_last(nx, kx_end, k1)
    esend1[0], esend1[1], esend1[2] = xs[end], p0[end], ix[end]
    esend1[3], esend1[4] = kx_end, 3.0 * iy[end] * di[end]
    pl.semaphore_wait(barrier, len(offsets))
    coming = [
        send(nsend1, nrecv1, 0, 1), send(esend1, erecv1, 1, 0),
        send(xs.at[0], xs.at[nx], -1, 0), send(xs.at[0], cx.at[0], -1, 1),
        send(strip.at[0], hy.at[0], 0, -1), send(strip.at[0], cy.at[0], 1, -1),
    ]

    column, flux = complete(0, xs, ys, zs, p0, coming, nrecv1, erecv1, nrecv1, erecv1)

    def body(i, held):
        flux, h0, s1, m0 = held
        fx, fy, fz, flux = column(i, flux)
        fx, fy, fz = -fx, -fy, -fz
        rx[i], ry[i], rz[i] = fx, fy, fz
        m0 = m0 + fold(fx * fx + fy * fy) + fold(fz * fz)
        return flux, pack_first(i, fy, h0), pack_last(i, fy, s1), m0

    flux, h0, s1, m0 = loop(body, (flux, zero, zero, zero8))
    strip[1] = h0
    nsend2[0] = s1
    esend2[0] = rx[end]
    coming = [
        send(rx.at[0], rx.at[nx], -1, 0), send(rx.at[0], cx.at[1], -1, 1),
        send(strip.at[1], hy.at[1], 0, -1), send(strip.at[1], cy.at[1], 1, -1),
    ]

    def body(i, q1):
        p = partial(i, rx, ry, rz, ix[i], iy[i], iz[i], di[i], None)
        p1[i] = p
        return pack_last(i, p, q1)

    q1 = loop(body, zero)
    nsend2[1] = q1
    esend2[1] = p1[end]
    coming += [send(esend2, erecv2, 1, 0), send(nsend2, nrecv2, 0, 1)]
    column, flux = complete(1, rx, ry, rz, p1, coming, nrecv2, erecv2, nrecv1, erecv1)

    def body(i, held):
        flux, h0, m1, m2 = held
        fx, fy, fz, flux = column(i, flux)
        vx[i], vy[i], vz[i] = fx, fy, fz
        m1 = m1 + fold(fx * rx[i] + fy * ry[i]) + fold(fz * rz[i])
        m2 = m2 + fold(fx * fx + fy * fy) + fold(fz * fz)
        return flux, pack_first(i, fy, h0), m1, m2

    flux, h0, m1, m2 = loop(body, (flux, zero, zero8, zero8))
    strip[2] = h0
    coming = [send(vx.at[0], vx.at[nx], -1, 0), send(strip.at[2], hy.at[2], 0, -1)]

    def body(i, held):
        s1, q1, m3 = held
        w, s = vx[i], vy[i]
        e = jnp.where(i < nx - 1, vx[jnp.minimum(i + 1, nx - 1)], 0.0)
        bottom, top = vz[i, pl.ds(0, levels), :], vz[i, pl.ds(1, levels), :]
        a, b, c = ix[i], iy[i], iz[i]
        n = jnp.where(last, 0.0, pltpu.roll(s, ny - 1, 1))
        sumx, sumy, sumz = w + e, s + n, bottom + top
        total = 3.0 * (a * sumx + b * sumy + c * sumz)
        p = total * di[i]
        p2[i] = p
        energy = (
            a * (w * w + e * e + sumx * sumx)
            + b * (s * s + n * n + sumy * sumy)
            + c * (bottom * bottom + top * top + sumz * sumz)
            - p * total
        )
        return pack_last(i, s, s1), pack_last(i, p, q1), m3 + fold(energy)

    s1, q1, m3 = loop(body, (zero, zero, zero8))
    for copy in coming:
        copy.wait_recv()
    e = vx[nx]
    grow = kx_end * e
    m3 = m3 + fold(ix[end] * e * (2.0 * (e + vx[end]) - 6.0 * p2[end] - 3.0 * grow))
    p2[end] = p2[end] + grow
    n = hy[2]
    q1 = q1 + jnp.where(lane == end, pltpu.roll(grow, nx, 1), 0.0)
    grow = nsend1[3] * n
    rest = nsend1[2] * n * (2.0 * (n + s1) - 6.0 * q1 - 3.0 * grow)
    m3 = m3 + fold(jnp.where(lane < nx, rest, 0.0))
    row_grow = jnp.where(lane < nx, grow, 0.0)

    row = lax.broadcasted_iota(jnp.int32, (8, ny), 0)
    mine = zero8
    for n, m in enumerate((m0, m1, m2, m3)):
        mine = jnp.where(row == n, jnp.sum(m, 0, keepdims=True), mine)
    mom[0] = mine
    if direct:
        others = [(a, b) for a in range(npx) for b in range(npy)][1:]
        for n, (a, b) in enumerate(others):
            copy = pltpu.make_async_remote_copy(
                src_ref=mom.at[0], dst_ref=slots1.at[n], send_sem=send_sem.at[14 + n],
                recv_sem=all_sem, device_id=device(a, b), device_id_type=MESH,
            )
            copy.start()
            sent.append(copy)
        whole = slots1.at[pl.ds(0, len(others))]
        pltpu.make_async_copy(whole, whole, all_sem).wait()
        mine = mine + jnp.sum(slots1[: len(others)], 0)
    else:
        coming = [send(mom.at[0], slots1.at[d], d, 0) for d in range(1, npx)]
        for d, copy in enumerate(coming):
            copy.wait_recv()
            mine = mine + slots1[d + 1]
        mom[1] = mine
        coming = [send(mom.at[1], slots2.at[d], 0, d) for d in range(1, npy)]
        for d, copy in enumerate(coming):
            copy.wait_recv()
            mine = mine + slots2[d + 1]
    mine = jnp.sum(mine, 1, keepdims=True)
    m0, m1, m2, m3 = mine[0:1], mine[1:2], mine[2:3], mine[3:4]
    a0 = m0 / m1
    new = a0 * a0 * m2 - m0
    grown = 1.0 + new / m0
    curve = a0 * (a0 * m3 - grown * m2)
    good = (new > 0.0) & (curve > 0.0)
    a1 = jnp.where(good, new / jnp.where(good, curve, 1.0), 0.0)
    c0 = a0 + a1 * grown
    c1 = -a0 * a1
    c0 = jnp.broadcast_to(c0, (1, ny))
    c1 = jnp.broadcast_to(c1, (1, ny))

    stores = []

    def store(n, source, target):
        copy = pltpu.make_async_copy(source, target, out_sem.at[n])
        copy.start()
        stores.append(copy)

    def body(i, carry):
        faces = pl.ds(0, levels + 1)
        zs[i] = zs[i] + c0 * rz[i, faces, :] + c1 * vz[i, faces, :]
        return carry

    loop(body, 0)
    for level in range(levels + 1):
        store(3 + level, zs.at[:, level, :], oz.at[level])
    for n, (made, base, once, twice, target) in enumerate(
        ((ix, xs, rx, vx, ox), (iy, ys, ry, vy, oy))
    ):

        def body(i, carry):
            made[i] = base[i] + c0 * once[i] + c1 * twice[i]
            return carry

        loop(body, 0)
        store(n, made, target)

    def body(i, carry):
        halo = pltpu.roll(row_grow, ny - 1 - i, 1)
        iz[i] = p0[i] + c0 * p1[i] + c1 * (p2[i] + jnp.where(last, halo, 0.0))
        return carry

    loop(body, 0)
    store(2, iz, op)
    for copy in stores:
        copy.wait()
    for copy in sent:
        copy.wait_send()


def local(npx, npy, metric, helmholtz, forcing, orientation, start_x, start_y, start_z):
    nx, levels, ny = start_x.shape
    faces = levels + 8
    cells = pltpu.VMEM((nx, levels, ny), F32)
    padded = pltpu.VMEM((nx + 1, levels, ny), F32)
    vertical = pltpu.VMEM((nx, faces, ny), F32)

    def tiles(n):
        return pltpu.VMEM((n, levels, ny), F32)

    direct = npx * npy <= DIRECT
    sends = 14 + (npx * npy - 1 if direct else npx + npy - 2)
    start_z = jnp.swapaxes(start_z, 0, 1)
    x, y, z, pressure = pl.pallas_call(
        functools.partial(kernel, npx, npy),
        out_shape=[jax.ShapeDtypeStruct(a.shape, F32) for a in (start_x, start_y, start_z, start_x)],
        in_specs=[pl.BlockSpec(memory_space=pltpu.HBM)] * 7,
        out_specs=[pl.BlockSpec(memory_space=pl.ANY)] * 4,
        scratch_shapes=[
            pltpu.VMEM(metric.shape, metric.dtype),
            pltpu.VMEM(helmholtz.shape, helmholtz.dtype),
            pltpu.VMEM(forcing.shape, forcing.dtype),
            pltpu.VMEM(orientation.shape, orientation.dtype),
            padded, cells, pltpu.VMEM((nx, levels + 1, ny), F32),
            cells, cells, cells, cells, cells, cells, cells,
            padded, cells, vertical, padded, cells, vertical,
            tiles(3), tiles(4), tiles(5), tiles(2), tiles(2),
            tiles(3), tiles(2), tiles(2), tiles(4), tiles(5), tiles(2), tiles(2),
            pltpu.VMEM((2, 8, ny), F32),
            pltpu.VMEM((npx * npy if direct else npx, 8, ny), F32),
            pltpu.VMEM((npy, 8, ny), F32),
            pltpu.SemaphoreType.DMA((6,)),
            pltpu.SemaphoreType.DMA((levels + 1,)),
            pltpu.SemaphoreType.DMA((levels + 4,)),
            pltpu.SemaphoreType.DMA((sends,)),
            pltpu.SemaphoreType.DMA((sends,)),
            pltpu.SemaphoreType.DMA,
        ],
        compiler_params=pltpu.CompilerParams(
            collective_id=0, has_side_effects=True, vmem_limit_bytes=40 * 1024 * 1024
        ),
    )(*[pltpu.with_memory_space_constraint(a, pltpu.HBM) for a in (metric, helmholtz, forcing, orientation, start_x, start_y, start_z)])
    return x, y, jnp.swapaxes(z, 0, 1), pressure


def solution(mesh):
    return jax.shard_map(
        functools.partial(local, mesh.shape["px"], mesh.shape["py"]),
        mesh=mesh,
        in_specs=(
            P(None, "px", None, "py"),
            P("px", None, "py"),
            P("px", None, "py"),
            P("px", "py"),
            P("px", None, "py"),
            P("px", None, "py"),
            P("px", None, "py"),
        ),
        out_specs=(P("px", None, "py"),) * 4,
        check_vma=False,
    )
```
